32 devices in a mesh: rep: 2 (over x), dp: 16 (over y, z, core).
Axes of the slice: x: 2, y: 2, z: 4, core: 2. Of those that a mesh axis runs over, the one named last changes fastest.
Arguments:
- x: bfloat16 [32, 2048, 640], P(('rep', 'dp')), parts along dimension 0
- dy: bfloat16 [32, 2048, 640], P(('rep', 'dp')), parts along dimension 0
- w_gate: bfloat16 [2, 640, 2048], replicated
- w_up: bfloat16 [2, 640, 2048], replicated
- w_down: bfloat16 [2, 2048, 640], replicated
- m_w_gate: float32 [2, 640, 2048], replicated
- m_w_up: float32 [2, 640, 2048], replicated
- m_w_down: float32 [2, 2048, 640], replicated
- v_w_gate: float32 [2, 640, 2048], replicated
- v_w_up: float32 [2, 640, 2048], replicated
- v_w_down: float32 [2, 2048, 640], replicated
Outputs:
- output 1: bfloat16 [4, 640, 2048], P('rep'), parts along dimension 0
- output 2: bfloat16 [4, 640, 2048], P('rep'), parts along dimension 0
- output 3: bfloat16 [4, 2048, 640], P('rep'), parts along dimension 0
- output 4: float32 [4, 640, 2048], P('rep'), parts along dimension 0
- output 5: float32 [4, 640, 2048], P('rep'), parts along dimension 0
- output 6: float32 [4, 2048, 640], P('rep'), parts along dimension 0
- output 7: float32 [4, 640, 2048], P('rep'), parts along dimension 0
- output 8: float32 [4, 640, 2048], P('rep'), parts along dimension 0
- output 9: float32 [4, 2048, 640], P('rep'), parts along dimension 0
There are 2 independent parts. The reference program is written for one: setup_inputs(seed, part) draws one part's arguments, and reference() takes and returns one part's arrays. A program takes and returns all parts, laid end to end along the dimension named above; an argument that names none is the same for every part.
All inputs are finite; a program needn't handle non-finite values.
Results may differ from the reference program's by a relative error of at most 0.022.
Values are sent between devices in bfloat16 or wider.
A program may use at most 2.25 GiB of HBM per device.

```python
import jax
import jax.numpy as jnp
from jax import lax

SEQUENCES = 16
TOKENS = 2048
D = 640
FF = 2048
LAYERS = 2
NAMES = ("w_gate", "w_up", "w_down")
SHAPES = {"w_gate": (LAYERS, D, FF), "w_up": (LAYERS, D, FF), "w_down": (LAYERS, FF, D)}


def bump(key, n, height):
    away = (jnp.arange(n, dtype=jnp.int32) - jax.random.randint(key, (), 0, n, jnp.int32)) % n
    return jnp.where(away < n // 8, height, 1.0)


def together(key, own, strength):
    shared = jax.random.normal(key, own.shape[1:], jnp.float32)
    return (own + strength * shared) * lax.rsqrt(1 + strength * strength)


def setup_inputs(seed: int = 0, part: int = 0) -> dict:
    kx, kdy, ka, kb, kz, kf, kh, kl, *keys = jax.random.split(jax.random.key(seed), 8 + 3 * len(NAMES))
    kx, kdy, ka, kb = (jax.random.fold_in(k, part) for k in (kx, kdy, ka, kb))
    kw, km, kv = (keys[i::3] for i in range(3))
    shape = (SEQUENCES, TOKENS, D)
    much_x, much_dy = jax.random.uniform(kz, (2,), jnp.float32, 0.0, 1.0)
    loud = 2.0 ** jax.random.uniform(jax.random.fold_in(kz, 1), (), jnp.float32, -1.0, 2.0)
    layers = 2.0 ** jax.random.uniform(kl, (LAYERS, 1, 1), jnp.float32, -1.0, 1.0)
    x = together(ka, jax.random.normal(kx, shape, jnp.float32), much_x) * bump(kf, D, 4.0)
    dy = together(kb, jax.random.normal(kdy, shape, jnp.float32), much_dy)
    drawn = {"x": x.astype(jnp.bfloat16), "dy": (loud * dy * (SEQUENCES * TOKENS) ** -0.5).astype(jnp.bfloat16)}
    for key, name in zip(kw, NAMES, strict=True):
        w = jax.random.normal(key, SHAPES[name], jnp.float32) * SHAPES[name][1] ** -0.5
        drawn[name] = (w * {"w_gate": 1.0, "w_up": bump(kh, FF, 4.0), "w_down": layers}[name]).astype(jnp.bfloat16)
    for key, name in zip(km, NAMES, strict=True):
        drawn[f"m_{name}"] = 0.1 * jax.random.normal(key, SHAPES[name], jnp.float32)
    for key, name in zip(kv, NAMES, strict=True):
        drawn[f"v_{name}"] = jax.random.uniform(key, SHAPES[name], jnp.float32, 0.005, 0.015)
    return drawn


def matmul(a, w):
    return jnp.dot(a, w, preferred_element_type=jnp.float32).astype(jnp.bfloat16)


def normed(h):
    wide = h.astype(jnp.float32)
    scale = lax.rsqrt(jnp.mean(wide**2, -1, keepdims=True) + 1e-6)
    return (wide * scale).astype(jnp.bfloat16)


def layer(h, w):
    a = normed(h)
    gate = jnp.dot(a, w["w_gate"], preferred_element_type=jnp.float32)
    up = jnp.dot(a, w["w_up"], preferred_element_type=jnp.float32)
    return h + matmul((jax.nn.silu(gate) * up).astype(jnp.bfloat16), w["w_down"])


def adamw(w, m, v, g):
    m = 0.9 * m + 0.1 * g
    v = 0.95 * v + 0.05 * g * g
    step = m * lax.rsqrt(v + 1e-8) + 0.1 * w
    return (w - 0.02 * step).astype(jnp.bfloat16), m, v


def clipped(gradients, sum_of_squares, count):
    factor = jnp.minimum(1.0, 0.5 * lax.rsqrt(sum_of_squares / count + 1e-30))
    return [g * factor for g in gradients]


def stack(weights, h):
    return lax.scan(lambda h, w: (layer(h, w), None), h, weights)[0]


def reference(x, dy, w_gate, w_up, w_down, m_w_gate, m_w_up, m_w_down, v_w_gate, v_w_up, v_w_down):
    weights = dict(zip(NAMES, (w_gate, w_up, w_down), strict=True))

    def take(so_far, sequence):
        h, by_y = sequence
        _, back = jax.vjp(lambda w: stack(w, h), weights)
        return jax.tree.map(lambda total, term: total + term.astype(jnp.float32), so_far, back(by_y)[0]), None

    none_yet = {name: jnp.zeros(w.shape, jnp.float32) for name, w in weights.items()}
    by_weights, _ = lax.scan(take, none_yet, (x, dy))
    gradients = [by_weights[name].astype(jnp.bfloat16).astype(jnp.float32) for name in NAMES]
    gradients = clipped(gradients, sum(jnp.sum(g * g) for g in gradients), sum(g.size for g in gradients))
    new = [
        adamw(w.astype(jnp.float32), m, v, g)
        for w, m, v, g in zip((w_gate, w_up, w_down), (m_w_gate, m_w_up, m_w_down), (v_w_gate, v_w_up, v_w_down), gradients, strict=True)
    ]
    return tuple(one[which] for which in range(3) for one in new)
```

```python
import jax
import jax.numpy as jnp
from jax import lax
from jax.experimental import pallas as pl
from jax.experimental.pallas import tpu as pltpu
from jax.sharding import PartitionSpec as P

T, D, FF, LAYERS = 2048, 640, 2048, 2
RING = 8
TILE = FF // RING
HALF = D // 2
ROWS = 512
BF, F32 = jnp.bfloat16, jnp.float32
MESH = pl.DeviceIdType.MESH


def dot(a, b, ca, cb):
    return lax.dot_general(a, b, (((ca,), (cb,)), ((), ())), preferred_element_type=F32)


def step_kernel(
    x_hbm, dy_hbm, wg_hbm, wu_hbm, wd_hbm, g_out, ss_out,
    H, A, AT, DY, DYT, ACC, HID, DG, DU, WG, WU, WD, G, R, L, PS,
    wsem, xsem, osem, p_s, p_r, rs_s, rs_r, ag_s, ag_r, ap_s, ap_r, free,
):
    me = lax.axis_index("dp")
    core = me % 2
    y, z = me // 8, (me // 2) % 4
    pos = z + y * (7 - 2 * z)

    def device(position, c):
        yy = position // 4
        zz = position - yy * (2 * position - 7)
        return {"dp": yy * 8 + zz * 2 + c}

    partner = device(pos, 1 - core)

    def chunk(k):
        return (pos + 8 + (4 - (k + 1) // 2) * (2 * (k % 2) - 1)) % RING

    def weight_copies(layer, k):
        at = pl.ds(pl.multiple_of(chunk(k) * TILE, TILE), TILE)
        slot = k % 2
        return (
            pltpu.make_async_copy(wg_hbm.at[layer, :, at], WG.at[slot], wsem.at[slot, 0]),
            pltpu.make_async_copy(wu_hbm.at[layer, :, at], WU.at[slot], wsem.at[slot, 1]),
            pltpu.make_async_copy(wd_hbm.at[layer, at, :], WD.at[slot], wsem.at[slot, 2]),
        )

    def start_weights(layer, k):
        for c in weight_copies(layer, k):
            c.start()

    def next_weights(layer, k):
        for c in weight_copies(layer, k):
            c.wait()

        @pl.when(k < RING - 1)
        def _():
            start_weights(layer, k + 1)

    x_copy = pltpu.make_async_copy(x_hbm, H, xsem.at[0])
    dy_copy = pltpu.make_async_copy(dy_hbm, DY, xsem.at[1])
    x_copy.start()
    dy_copy.start()
    start_weights(0, 0)

    barrier = pltpu.get_barrier_semaphore()
    for other in (partner, device((pos + 1) % RING, core), device((pos + 7) % RING, core)):
        pl.semaphore_signal(barrier, inc=1, device_id=other, device_id_type=MESH)
    pl.semaphore_wait(barrier, 3)

    def rows(r, n=ROWS):
        return pl.ds(pl.multiple_of(r * n, n), n)

    def normed_into(dst):
        @pl.loop(0, T // 128)
        def _(r):
            at = rows(r, 128)
            wide = H[at, :].astype(F32)
            scale = lax.rsqrt(jnp.mean(wide * wide, -1, keepdims=True) + 1e-6)
            dst[at, :] = (wide * scale).astype(BF)

    def transposed_into(dst, src):
        @pl.loop(0, T // 128)
        def _(r):
            at = rows(r, 128)
            dst[:, at] = src[at, :].T

    def partner_copy(layer, k):
        p = chunk(k)
        return pltpu.make_async_remote_copy(
            src_ref=G.at[layer, p, 1 - core], dst_ref=R.at[layer, p],
            send_sem=p_s.at[layer, k], recv_sem=p_r.at[layer, k], device_id=partner, device_id_type=MESH,
        )

    def ring_copy(layer, k, sign):
        return pltpu.make_async_remote_copy(
            src_ref=R.at[layer, chunk(k)], dst_ref=L.at[layer, k],
            send_sem=rs_s.at[layer, k], recv_sem=rs_r.at[layer, k],
            device_id=device((pos + RING + sign) % RING, core), device_id_type=MESH,
        )

    def add_up(layer, k, came, dst):
        p = chunk(k)
        for m in range(3):

            @pl.loop(0, HALF // 64)
            def _(r):
                at = rows(r, 64)
                total = G[layer, p, core, m, at, :].astype(F32) + R[layer, p, m, at, :].astype(F32)
                for j in came:
                    total += L[layer, j, m, at, :].astype(F32)
                dst[layer, p, m, at, :] = total.astype(BF)

    def reduce_step(layer, k):
        partner_copy(layer, k).wait()
        first = (k == 0) | ((k == 1) & (core == 1)) | ((k == 2) & (core == 0))
        late = k >= 3

        @pl.when(first)
        def _():
            add_up(layer, k, (), R)

        @pl.when((k == 1) & (core == 0) | (k == 2) & (core == 1))
        def _():
            ring_copy(layer, 0, 1).wait_recv()
            add_up(layer, k, (0,), R)

        @pl.when(late)
        def _():
            ring_copy(layer, k - 2, 1).wait_recv()
            add_up(layer, k, (k - 2,), R)

        @pl.when(k == 0)
        def _():
            ring_copy(layer, k, 1 - 2 * core).start()

        @pl.when(k > 0)
        def _():
            ring_copy(layer, k, 2 * (k % 2) - 1).start()

    def reduce_last(layer):
        partner_copy(layer, 7).wait()
        pl.semaphore_signal(free.at[layer], inc=1, device_id=partner, device_id_type=MESH)
        ring_copy(layer, 5, 1).wait_recv()
        ring_copy(layer, 6, 1).wait_recv()
        for m in range(3):

            @pl.loop(0, HALF // 64)
            def _(r):
                at = rows(r, 64)
                total = G[layer, pos, core, m, at, :].astype(F32) + R[layer, pos, m, at, :].astype(F32)
                total += L[layer, 5, m, at, :].astype(F32)
                total += L[layer, 6, m, at, :].astype(F32)
                G[layer, pos, core, m, at, :] = total.astype(BF)

        pl.semaphore_wait(free.at[layer], 1)

    def event_chunk(e):
        return (pos + 8 + ((e + 1) // 2) * (1 - 2 * (e % 2))) % RING

    def gather_copy(layer, e, m, p, sign):
        return pltpu.make_async_remote_copy(
            src_ref=G.at[layer, p, core, m], dst_ref=G.at[layer, p, core, m],
            send_sem=ag_s.at[layer, e, m], recv_sem=ag_r.at[layer, e, m],
            device_id=device((pos + RING + sign) % RING, core), device_id_type=MESH,
        )

    def share_copy(layer, e, c):
        p = event_chunk(e)
        return pltpu.make_async_remote_copy(
            src_ref=G.at[layer, p, c], dst_ref=G.at[layer, p, c],
            send_sem=ap_s.at[layer, e], recv_sem=ap_r.at[layer, e], device_id=partner, device_id_type=MESH,
        )

    def gather_event(layer, e):
        p = event_chunk(e)

        @pl.when(e == 0)
        def _():
            for m in range(3):
                gather_copy(layer, 1, m, p, 1).start()
                gather_copy(layer, 2, m, p, -1).start()

        @pl.when(e > 0)
        def _():
            for m in range(3):
                gather_copy(layer, e, m, p, 1).wait_recv()

                @pl.when((e <= 4) | ((e == 5) & (core == 0)))
                def _():
                    gather_copy(layer, e + 2, m, p, 2 * (e % 2) - 1).start()

                @pl.when((e == 6) & (core == 1))
                def _():
                    gather_copy(layer, 7, m, p, -1).start()

        share_copy(layer, e, core).start()

    def out_copy(layer, e):
        p = event_chunk(e)
        return pltpu.make_async_copy(G.at[layer, p], g_out.at[layer, p], osem.at[layer, e])

    def squares(layer, e):
        share_copy(layer, e, 1 - core).wait_recv()
        out_copy(layer, e).start()
        p = event_chunk(e)
        total = jnp.zeros((8, TILE), F32)
        for c in range(2):
            for m in range(3):

                def add(r, total):
                    wide = G[layer, p, c, m, rows(r, 64), :].astype(F32)
                    return total + jnp.sum((wide * wide).reshape(8, 8, TILE), 0)

                total = lax.fori_loop(0, HALF // 64, add, total)
        PS[layer, p] = total

    x_copy.wait()
    normed_into(A)

    @pl.loop(0, RING)
    def _(k):
        next_weights(0, k)
        slot = k % 2

        @pl.loop(0, T // ROWS)
        def _(r):
            at = rows(r)
            gate = dot(A[at, :], WG[slot], 1, 0)
            up = dot(A[at, :], WU[slot], 1, 0)
            hid = (gate * jax.nn.sigmoid(gate) * up).astype(BF)
            part = dot(hid, WD[slot], 1, 0)

            @pl.when(k == 0)
            def _():
                ACC[at, :] = part

            @pl.when(k > 0)
            def _():
                ACC[at, :] += part

    start_weights(1, 0)

    @pl.loop(0, T // 128)
    def _(r):
        at = rows(r, 128)
        H[at, :] = (H[at, :].astype(F32) + ACC[at, :].astype(BF).astype(F32)).astype(BF)

    normed_into(A)
    transposed_into(AT, A)
    dy_copy.wait()
    transposed_into(DYT, DY)

    def tile(layer, k):
        next_weights(layer, k)
        slot = k % 2

        @pl.loop(0, T // ROWS)
        def _(r):
            at = rows(r)
            gate = dot(A[at, :], WG[slot], 1, 0)
            up = dot(A[at, :], WU[slot], 1, 0)
            by_hid = dot(DY[at, :], WD[slot], 1, 1).astype(BF).astype(F32)
            sig = jax.nn.sigmoid(gate)
            silu = gate * sig
            HID[at, :] = (silu * up).astype(BF)
            by_up = (by_hid * silu).astype(BF)
            by_gate = (by_hid * up * (sig + silu * (1.0 - sig))).astype(BF)
            DU[at, :] = by_up
            DG[at, :] = by_gate
            if layer == 1:
                part = dot(by_gate, WG[slot], 1, 1) + dot(by_up, WU[slot], 1, 1)

                @pl.when(k == 0)
                def _():
                    ACC[at, :] = part

                @pl.when(k > 0)
                def _():
                    ACC[at, :] += part

        p = chunk(k)
        for m, left, right in ((0, AT, DG), (1, AT, DU), (2, DYT, HID)):

            @pl.loop(0, 2)
            def _(half):
                g = dot(left[rows(half, HALF), :], right[...], 1, 0)
                G[layer, p, half, m] = g.astype(BF)

        partner_copy(layer, k).start()

    @pl.loop(0, RING)
    def _(k):
        tile(1, k)

        @pl.when(k > 0)
        def _():
            reduce_step(1, k - 1)

    start_weights(0, 0)

    @pl.loop(0, T // 128)
    def _(r):
        at = rows(r, 128)
        by_a = ACC[at, :].astype(BF).astype(F32)
        wide = H[at, :].astype(F32)
        scale = lax.rsqrt(jnp.mean(wide * wide, -1, keepdims=True) + 1e-6)
        along = jnp.mean(by_a * wide, -1, keepdims=True) * (scale * scale)
        by_h = (scale * (by_a - wide * along)).astype(BF).astype(F32)
        DY[at, :] = (DY[at, :].astype(F32) + by_h).astype(BF)

    again = pltpu.make_async_copy(x_hbm, H, xsem.at[0])
    again.start()
    transposed_into(DYT, DY)
    again.wait()
    normed_into(A)
    transposed_into(AT, A)
    reduce_last(1)


    @pl.loop(0, RING)
    def _(k):
        tile(0, k)

        @pl.when(k > 0)
        def _():
            reduce_step(0, k - 1)

        gather_event(1, k)

    reduce_last(0)

    @pl.loop(0, RING)
    def _(e):
        gather_event(0, e)
        squares(1, e)

    @pl.loop(0, RING)
    def _(e):
        squares(0, e)

    total = jnp.zeros((8, TILE), F32)
    for layer in range(LAYERS):
        for p in range(RING):
            total += PS[layer, p]
    ss_out[...] = total

    for layer in range(LAYERS):

        @pl.loop(0, RING)
        def _(k):
            share_copy(layer, k, core).wait_send()
            out_copy(layer, k).wait()

        @pl.loop(0, RING - 1)
        def _(k):
            ring_copy(layer, k, 1).wait_send()
            for m in range(3):
                gather_copy(layer, k + 1, m, event_chunk(k + 1), 1).wait_send()


def update_kernel(ss, g, *refs):
    ins, outs = refs[:9], refs[9:]
    count = float(3 * LAYERS * D * FF)
    factor = jnp.minimum(1.0, 0.5 * lax.rsqrt(jnp.sum(ss[...]) / count + 1e-30))
    for i in range(3):
        w, m, v = ins[3 * i : 3 * i + 3]
        new_w, new_m, new_v = outs[3 * i : 3 * i + 3]
        grad = g[0, 0, :, i].reshape(D, TILE).astype(F32) * factor
        if i == 2:
            grad = grad.T
        mm = 0.9 * m[0] + 0.1 * grad
        vv = 0.95 * v[0] + 0.05 * grad * grad
        wide = w[0].astype(F32)
        new_m[0] = mm
        new_v[0] = vv
        new_w[0] = (wide - 0.02 * (mm * lax.rsqrt(vv + 1e-8) + 0.1 * wide)).astype(BF)


def solution(mesh):
    any_ = pl.BlockSpec(memory_space=pl.ANY)
    chunk_of = (3, HALF, TILE)
    dma = pltpu.SemaphoreType.DMA

    gradients = pl.pallas_call(
        step_kernel,
        name="gradients",
        out_shape=(
            jax.ShapeDtypeStruct((LAYERS, RING, 2, *chunk_of), BF),
            jax.ShapeDtypeStruct((8, TILE), F32),
        ),
        in_specs=[any_] * 5,
        out_specs=(any_, pl.BlockSpec(memory_space=pltpu.VMEM)),
        scratch_shapes=[
            pltpu.VMEM((T, D), BF), pltpu.VMEM((T, D), BF), pltpu.VMEM((D, T), BF), pltpu.VMEM((T, D), BF), pltpu.VMEM((D, T), BF),
            pltpu.VMEM((T, D), F32),
            pltpu.VMEM((T, TILE), BF), pltpu.VMEM((T, TILE), BF), pltpu.VMEM((T, TILE), BF),
            pltpu.VMEM((2, D, TILE), BF), pltpu.VMEM((2, D, TILE), BF), pltpu.VMEM((2, TILE, D), BF),
            pltpu.VMEM((LAYERS, RING, 2, *chunk_of), BF),
            pltpu.VMEM((LAYERS, RING, *chunk_of), BF),
            pltpu.VMEM((LAYERS, RING - 1, *chunk_of), BF),
            pltpu.VMEM((LAYERS, RING, 8, TILE), F32),
            dma((2, 3)), dma((2,)), dma((LAYERS, RING)),
            dma((LAYERS, RING)), dma((LAYERS, RING)),
            dma((LAYERS, RING - 1)), dma((LAYERS, RING - 1)),
            dma((LAYERS, RING, 3)), dma((LAYERS, RING, 3)),
            dma((LAYERS, RING)), dma((LAYERS, RING)), pltpu.SemaphoreType.REGULAR((LAYERS,)),
        ],
        compiler_params=pltpu.CompilerParams(collective_id=0, has_side_effects=True, vmem_limit_bytes=67_043_328),
    )

    wide = pl.BlockSpec((1, D, TILE), lambda l, p: (l, 0, p))
    tall = pl.BlockSpec((1, TILE, D), lambda l, p: (l, p, 0))
    specs = [wide] * 6 + [tall] * 3
    up_shape, down_shape = (LAYERS, D, FF), (LAYERS, FF, D)
    shapes = [jax.ShapeDtypeStruct(s, t) for s in (up_shape, up_shape, down_shape) for t in (BF, F32, F32)]
    update = pl.pallas_call(
        update_kernel,
        name="update",
        grid=(LAYERS, RING),
        out_shape=shapes,
        in_specs=[pl.BlockSpec((8, TILE), lambda l, p: (0, 0)), pl.BlockSpec((1, 1, 2, *chunk_of), lambda l, p: (l, p, 0, 0, 0, 0))] + specs,
        out_specs=specs,
        compiler_params=pltpu.CompilerParams(vmem_limit_bytes=60_000_000),
    )

    def step(x, dy, wg, wu, wd, mg, mu, md, vg, vu, vd):
        g, ss = gradients(x[0], dy[0], wg, wu, wd)
        new = update(ss, g, wg, mg, vg, wu, mu, vu, wd, md, vd)
        return tuple(new[3 * i + which] for which in range(3) for i in range(3))

    return jax.shard_map(
        step,
        mesh=mesh,
        in_specs=(P(("rep", "dp"), None, None),) * 2 + (P(None, None, None),) * 9,
        out_specs=(P("rep", None, None),) * 9,
        check_vma=False,
    )
```

```python
import jax
import jax.numpy as jnp
from jax import lax
from jax.experimental import pallas as pl
from jax.experimental.pallas import tpu as pltpu
from jax.sharding import PartitionSpec as P

T, D, FF, LAYERS = 2048, 640, 2048, 2
RING = 8
TILE = FF // RING
HALF = D // 2
SUB = TILE // 2
PARTS = 2 * LAYERS
ROWS, FEW = 1024, 512
BF, F32 = jnp.bfloat16, jnp.float32
MESH = pl.DeviceIdType.MESH


def dot(a, b, ca, cb):
    return lax.dot_general(a, b, (((ca,), (cb,)), ((), ())), preferred_element_type=F32)


def step_kernel(
    x_hbm, dy_hbm, wg_hbm, wu_hbm, wd_hbm, g_out, ss_out,
    H, A, AT, DY, DYT, ACC, HID, DGU, WGU, WD, G, R, L, PS,
    wsem, xsem, osem, p_s, p_r, rs_s, rs_r, ag_s, ag_r, ap_s, ap_r, free,
):
    me = lax.axis_index("dp")
    core = me % 2
    y, z = me // 8, (me // 2) % 4
    pos = z + y * (7 - 2 * z)

    def device(position, c):
        yy = position // 4
        zz = position - yy * (2 * position - 7)
        return {"dp": yy * 8 + zz * 2 + c}

    partner = device(pos, 1 - core)

    def chunk(k):
        return (pos + 8 + (4 - (k + 1) // 2) * (2 * (k % 2) - 1)) % RING

    def weight_copies(layer, n):
        slot, half = n % 2, n // 4
        copies = []
        for j in range(2):
            at = pl.ds(pl.multiple_of(chunk((2 * n + j) % RING) * TILE + half * SUB, SUB), SUB)
            here = pl.ds(j * SUB, SUB)
            copies += [
                pltpu.make_async_copy(wg_hbm.at[layer, :, at], WGU.at[slot, :, here], wsem.at[slot, 3 * j]),
                pltpu.make_async_copy(wu_hbm.at[layer, :, at], WGU.at[slot, :, pl.ds(TILE + j * SUB, SUB)], wsem.at[slot, 3 * j + 1]),
                pltpu.make_async_copy(wd_hbm.at[layer, at, :], WD.at[slot, here, :], wsem.at[slot, 3 * j + 2]),
            ]
        return copies

    def start_weights(layer, k):
        for c in weight_copies(layer, k):
            c.start()

    def next_weights(layer, k):
        for c in weight_copies(layer, k):
            c.wait()

        @pl.when(k < RING - 1)
        def _():
            start_weights(layer, k + 1)

    x_copy = pltpu.make_async_copy(x_hbm, H, xsem.at[0])
    dy_copy = pltpu.make_async_copy(dy_hbm, DY, xsem.at[1])
    x_copy.start()
    dy_copy.start()
    start_weights(0, 0)

    barrier = pltpu.get_barrier_semaphore()
    for other in (partner, device((pos + 1) % RING, core), device((pos + 7) % RING, core)):
        pl.semaphore_signal(barrier, inc=1, device_id=other, device_id_type=MESH)

    def rows(r, n=ROWS):
        return pl.ds(pl.multiple_of(r * n, n), n)

    def normed_into(dst):
        @pl.loop(0, T // FEW)
        def _(r):
            at = rows(r, FEW)
            wide = H[at, :].astype(F32)
            scale = lax.rsqrt(jnp.mean(wide * wide, -1, keepdims=True) + 1e-6)
            dst[at, :] = (wide * scale).astype(BF)

    def transposed_into(dst, src):
        @pl.loop(0, T // FEW)
        def _(r):
            at = rows(r, FEW)
            dst[:, at] = src[at, :].T

    def partner_copy(part, k):
        p = chunk(k)
        return pltpu.make_async_remote_copy(
            src_ref=G.at[part, p, 1 - core], dst_ref=R.at[part, p],
            send_sem=p_s.at[part, k], recv_sem=p_r.at[part, k], device_id=partner, device_id_type=MESH,
        )

    def ring_copy(part, k, sign):
        return pltpu.make_async_remote_copy(
            src_ref=R.at[part, chunk(k)], dst_ref=L.at[part, k],
            send_sem=rs_s.at[part, k], recv_sem=rs_r.at[part, k],
            device_id=device((pos + RING + sign) % RING, core), device_id_type=MESH,
        )

    def add_up(part, k, came, dst):
        p = chunk(k)
        for m in range(3):

            @pl.loop(0, HALF // 64)
            def _(r):
                at = rows(r, 64)
                total = G[part, p, core, m, at, :].astype(F32) + R[part, p, m, at, :].astype(F32)
                for j in came:
                    total += L[part, j, m, at, :].astype(F32)
                dst[part, p, m, at, :] = total.astype(BF)

    def reduce_step(part, k):
        partner_copy(part, k).wait()
        first = (k == 0) | ((k == 1) & (core == 1)) | ((k == 2) & (core == 0))
        late = k >= 3

        @pl.when(first)
        def _():
            add_up(part, k, (), R)

        @pl.when((k == 1) & (core == 0) | (k == 2) & (core == 1))
        def _():
            ring_copy(part, 0, 1).wait_recv()
            add_up(part, k, (0,), R)

        @pl.when(late)
        def _():
            ring_copy(part, k - 2, 1).wait_recv()
            add_up(part, k, (k - 2,), R)

        @pl.when(k == 0)
        def _():
            ring_copy(part, k, 1 - 2 * core).start()

        @pl.when(k > 0)
        def _():
            ring_copy(part, k, 2 * (k % 2) - 1).start()

    def reduce_last(part):
        partner_copy(part, 7).wait()
        pl.semaphore_signal(free.at[part], inc=1, device_id=partner, device_id_type=MESH)
        ring_copy(part, 5, 1).wait_recv()
        ring_copy(part, 6, 1).wait_recv()
        for m in range(3):

            @pl.loop(0, HALF // 64)
            def _(r):
                at = rows(r, 64)
                total = G[part, pos, core, m, at, :].astype(F32) + R[part, pos, m, at, :].astype(F32)
                total += L[part, 5, m, at, :].astype(F32)
                total += L[part, 6, m, at, :].astype(F32)
                G[part, pos, core, m, at, :] = total.astype(BF)

        pl.semaphore_wait(free.at[part], 1)

    def event_chunk(e):
        return (pos + 8 + ((e + 1) // 2) * (1 - 2 * (e % 2))) % RING

    def gather_copy(part, e, m, p, sign):
        return pltpu.make_async_remote_copy(
            src_ref=G.at[part, p, core, m], dst_ref=G.at[part, p, core, m],
            send_sem=ag_s.at[part, e, m], recv_sem=ag_r.at[part, e, m],
            device_id=device((pos + RING + sign) % RING, core), device_id_type=MESH,
        )

    def share_copy(part, e, c):
        p = event_chunk(e)
        return pltpu.make_async_remote_copy(
            src_ref=G.at[part, p, c], dst_ref=G.at[part, p, c],
            send_sem=ap_s.at[part, e], recv_sem=ap_r.at[part, e], device_id=partner, device_id_type=MESH,
        )

    def gather_event(part, e):
        p = event_chunk(e)

        @pl.when(e == 0)
        def _():
            for m in range(3):
                gather_copy(part, 1, m, p, 1).start()
                gather_copy(part, 2, m, p, -1).start()

        @pl.when(e > 0)
        def _():
            for m in range(3):
                gather_copy(part, e, m, p, 1).wait_recv()

                @pl.when((e <= 4) | ((e == 5) & (core == 0)))
                def _():
                    gather_copy(part, e + 2, m, p, 2 * (e % 2) - 1).start()

                @pl.when((e == 6) & (core == 1))
                def _():
                    gather_copy(part, 7, m, p, -1).start()

        share_copy(part, e, core).start()

    def out_copy(part, e):
        p = event_chunk(e)
        return pltpu.make_async_copy(G.at[part, p], g_out.at[part, p], osem.at[part, e])

    def squares(part, e):
        share_copy(part, e, 1 - core).wait_recv()
        out_copy(part, e).start()
        p = event_chunk(e)
        total = jnp.zeros((8, SUB), F32)
        for c in range(2):
            for m in range(3):

                def add(r, total):
                    wide = G[part, p, c, m, rows(r, 64), :].astype(F32)
                    return total + jnp.sum((wide * wide).reshape(8, 8, SUB), 0)

                total = lax.fori_loop(0, HALF // 64, add, total)
        PS[part, p] = total

    x_copy.wait()
    normed_into(A)

    @pl.loop(0, RING)
    def _(k):
        next_weights(0, k)
        slot = k % 2

        @pl.loop(0, T // ROWS)
        def _(r):
            at = rows(r)
            both = dot(A[at, :], WGU[slot], 1, 0)
            gate, up = both[:, :TILE], both[:, TILE:]
            hid = (gate * jax.nn.sigmoid(gate) * up).astype(BF)
            part = dot(hid, WD[slot], 1, 0)

            @pl.when(k == 0)
            def _():
                ACC[at, :] = part

            @pl.when(k > 0)
            def _():
                ACC[at, :] += part

    start_weights(1, 0)

    @pl.loop(0, T // FEW)
    def _(r):
        at = rows(r, FEW)
        H[at, :] = (H[at, :].astype(F32) + ACC[at, :].astype(BF).astype(F32)).astype(BF)

    normed_into(A)
    transposed_into(AT, A)
    dy_copy.wait()
    transposed_into(DYT, DY)

    def tile(part, n):
        layer = 1 - part // 2
        next_weights(layer, n)
        slot = n % 2

        @pl.loop(0, T // ROWS)
        def _(r):
            at = rows(r)
            both = dot(A[at, :], WGU[slot], 1, 0)
            gate, up = both[:, :TILE], both[:, TILE:]
            by_hid = dot(DY[at, :], WD[slot], 1, 1).astype(BF).astype(F32)
            sig = jax.nn.sigmoid(gate)
            silu = gate * sig
            HID[at, :] = (silu * up).astype(BF)
            DGU[at, pl.ds(TILE, TILE)] = (by_hid * silu).astype(BF)
            DGU[at, pl.ds(0, TILE)] = (by_hid * up * (sig + silu * (1.0 - sig))).astype(BF)

        if layer == 1:

            @pl.loop(0, T // ROWS)
            def _(r):
                at = rows(r)
                term = dot(DGU[at, :], WGU[slot], 1, 1)

                @pl.when(n == 0)
                def _():
                    ACC[at, :] = term

                @pl.when(n > 0)
                def _():
                    ACC[at, :] += term

        settle(part, n % 4)

        for left, right, ms in ((AT, DGU, (0, 1)), (DYT, HID, (2,))):
            g = dot(left[...], right[...], 1, 0).astype(BF)
            for i, m in enumerate(ms):
                for j in range(2):
                    at = slice(i * TILE + j * SUB, i * TILE + (j + 1) * SUB)
                    for half in range(2):
                        G[part, chunk((2 * n + j) % RING), half, m] = g[half * HALF : (half + 1) * HALF, at]

        for j in range(2):
            partner_copy(part, (2 * n + j) % RING).start()

    def settle(part, n):
        @pl.when(n == 0)
        def _():
            if part > 0:
                reduce_step(part - 1, 5)
                reduce_step(part - 1, 6)
            if part > 1:
                gather_event(part - 2, 5)
                gather_event(part - 2, 6)

        @pl.when(n == 1)
        def _():
            reduce_step(part, 0)
            if part > 0:
                reduce_last(part - 1)
                gather_event(part - 1, 0)
            if part > 1:
                gather_event(part - 2, 7)

        @pl.when(n > 1)
        def _():
            reduce_step(part, 2 * n - 3)
            reduce_step(part, 2 * n - 2)
            if part > 0:
                gather_event(part - 1, 2 * n - 3)
                gather_event(part - 1, 2 * n - 2)

    pl.semaphore_wait(barrier, 3)

    for part in range(2):

        @pl.loop(0, 4)
        def _(n):
            tile(part, 4 * part + n)

    start_weights(0, 0)

    @pl.loop(0, T // FEW)
    def _(r):
        at = rows(r, FEW)
        by_a = ACC[at, :].astype(BF).astype(F32)
        wide = H[at, :].astype(F32)
        scale = lax.rsqrt(jnp.mean(wide * wide, -1, keepdims=True) + 1e-6)
        along = jnp.mean(by_a * wide, -1, keepdims=True) * (scale * scale)
        by_h = (scale * (by_a - wide * along)).astype(BF).astype(F32)
        DY[at, :] = (DY[at, :].astype(F32) + by_h).astype(BF)

    again = pltpu.make_async_copy(x_hbm, H, xsem.at[0])
    again.start()
    transposed_into(DYT, DY)
    again.wait()
    normed_into(A)
    transposed_into(AT, A)

    for part in range(2, 4):

        @pl.loop(0, 4)
        def _(n):
            tile(part, 4 * (part - 2) + n)

    reduce_step(3, 5)
    reduce_step(3, 6)
    gather_event(2, 5)
    gather_event(2, 6)

    @pl.loop(0, RING)
    def _(e):
        for part in range(2):
            squares(part, e)

    reduce_last(3)
    gather_event(3, 0)
    gather_event(2, 7)

    @pl.loop(1, RING)
    def _(e):
        squares(2, e - 1)
        gather_event(3, e)
        squares(3, e - 1)

    squares(2, 7)
    squares(3, 7)

    total = jnp.zeros((8, SUB), F32)
    for part in range(PARTS):
        for p in range(RING):
            total += PS[part, p]
    ss_out[...] = total

    for part in range(PARTS):

        @pl.loop(0, RING)
        def _(k):
            share_copy(part, k, core).wait_send()
            out_copy(part, k).wait()

        @pl.loop(0, RING - 1)
        def _(k):
            ring_copy(part, k, 1).wait_send()
            for m in range(3):
                gather_copy(part, k + 1, m, event_chunk(k + 1), 1).wait_send()


def update_kernel(ss, g, *refs):
    ins, outs = refs[:9], refs[9:]
    count = float(3 * LAYERS * D * FF)
    factor = jnp.minimum(1.0, 0.5 * lax.rsqrt(jnp.sum(ss[...]) / count + 1e-30))
    for i in range(3):
        w, m, v = ins[3 * i : 3 * i + 3]
        new_w, new_m, new_v = outs[3 * i : 3 * i + 3]
        grad = jnp.concatenate([g[half, 0, :, i].reshape(D, SUB) for half in range(2)], 1).astype(F32) * factor
        if i == 2:
            grad = grad.T
        mm = 0.9 * m[0] + 0.1 * grad
        vv = 0.95 * v[0] + 0.05 * grad * grad
        wide = w[0].astype(F32)
        new_m[0] = mm
        new_v[0] = vv
        new_w[0] = (wide - 0.02 * (mm * lax.rsqrt(vv + 1e-8) + 0.1 * wide)).astype(BF)


def solution(mesh):
    any_ = pl.BlockSpec(memory_space=pl.ANY)
    chunk_of = (3, HALF, SUB)
    dma = pltpu.SemaphoreType.DMA

    gradients = pl.pallas_call(
        step_kernel,
        name="gradients",
        out_shape=(
            jax.ShapeDtypeStruct((PARTS, RING, 2, *chunk_of), BF),
            jax.ShapeDtypeStruct((8, SUB), F32),
        ),
        in_specs=[any_] * 5,
        out_specs=(any_, pl.BlockSpec(memory_space=pltpu.VMEM)),
        scratch_shapes=[
            pltpu.VMEM((T, D), BF), pltpu.VMEM((T, D), BF), pltpu.VMEM((D, T), BF), pltpu.VMEM((T, D), BF), pltpu.VMEM((D, T), BF),
            pltpu.VMEM((T, D), F32),
            pltpu.VMEM((T, TILE), BF), pltpu.VMEM((T, 2 * TILE), BF),
            pltpu.VMEM((2, D, 2 * TILE), BF), pltpu.VMEM((2, TILE, D), BF),
            pltpu.VMEM((PARTS, RING, 2, *chunk_of), BF),
            pltpu.VMEM((PARTS, RING, *chunk_of), BF),
            pltpu.VMEM((PARTS, RING - 1, *chunk_of), BF),
            pltpu.VMEM((PARTS, RING, 8, SUB), F32),
            dma((2, 6)), dma((2,)), dma((PARTS, RING)),
            dma((PARTS, RING)), dma((PARTS, RING)),
            dma((PARTS, RING - 1)), dma((PARTS, RING - 1)),
            dma((PARTS, RING, 3)), dma((PARTS, RING, 3)),
            dma((PARTS, RING)), dma((PARTS, RING)), pltpu.SemaphoreType.REGULAR((PARTS,)),
        ],
        compiler_params=pltpu.CompilerParams(collective_id=0, has_side_effects=True, vmem_limit_bytes=67_043_328),
    )

    wide = pl.BlockSpec((1, D, TILE), lambda l, p: (l, 0, p))
    tall = pl.BlockSpec((1, TILE, D), lambda l, p: (l, p, 0))
    specs = [wide] * 6 + [tall] * 3
    up_shape, down_shape = (LAYERS, D, FF), (LAYERS, FF, D)
    shapes = [jax.ShapeDtypeStruct(s, t) for s in (up_shape, up_shape, down_shape) for t in (BF, F32, F32)]
    update = pl.pallas_call(
        update_kernel,
        name="update",
        grid=(LAYERS, RING),
        out_shape=shapes,
        in_specs=[pl.BlockSpec((8, SUB), lambda l, p: (0, 0)), pl.BlockSpec((2, 1, 2, *chunk_of), lambda l, p: (1 - l, p, 0, 0, 0, 0))] + specs,
        out_specs=specs,
        compiler_params=pltpu.CompilerParams(vmem_limit_bytes=60_000_000),
    )

    def step(x, dy, wg, wu, wd, mg, mu, md, vg, vu, vd):
        g, ss = gradients(x[0], dy[0], wg, wu, wd)
        new = update(ss, g, wg, mg, vg, wu, mu, vu, wd, md, vd)
        return tuple(new[3 * i + which] for which in range(3) for i in range(3))

    return jax.shard_map(
        step,
        mesh=mesh,
        in_specs=(P(("rep", "dp"), None, None),) * 2 + (P(None, None, None),) * 9,
        out_specs=(P("rep", None, None),) * 9,
        check_vma=False,
    )
```

```python
import jax
import jax.numpy as jnp
from jax import lax
from jax.experimental import pallas as pl
from jax.experimental.pallas import tpu as pltpu
from jax.sharding import PartitionSpec as P

T, D, FF, LAYERS = 2048, 640, 2048, 2
RING = 8
TILE = FF // RING
HALF = D // 2
SUB = TILE // 2
PARTS = 2 * LAYERS
ROWS, FEW = 1024, 512
BF, F32 = jnp.bfloat16, jnp.float32
MESH = pl.DeviceIdType.MESH


def rem(a, b):
    return a % b if isinstance(a, int) else lax.rem(a, jnp.int32(b))


def div(a, b):
    return a // b if isinstance(a, int) else lax.div(a, jnp.int32(b))


def dot(a, b, ca, cb):
    return lax.dot_general(a, b, (((ca,), (cb,)), ((), ())), preferred_element_type=F32)


def step_kernel(
    x_hbm, dy_hbm, wg_hbm, wu_hbm, wd_hbm, g_out, ss_out, kept,
    H, A, AT, DY, DYT, ACC, HID, DGU, WGU, WD, G, R, L, PS,
    wsem, xsem, osem, ksem, p_s, p_r, rs_s, rs_r, ag_s, ag_r, ap_s, ap_r, free,
):
    me = lax.axis_index("dp")
    core = rem(me, 2)
    y, z = div(me, 8), rem(div(me, 2), 4)
    pos = z + y * (7 - 2 * z)

    def device(position, c):
        yy = div(position, 4)
        zz = position - yy * (2 * position - 7)
        return {"dp": yy * 8 + zz * 2 + c}

    partner = device(pos, 1 - core)

    def chunk(k):
        return rem(pos + 8 + (4 - div(k + 1, 2)) * (2 * rem(k, 2) - 1), RING)

    def weight_copies(layer, n):
        slot, half = rem(n, 2), div(n, 4)
        copies = []
        for j in range(2):
            at = pl.ds(pl.multiple_of(chunk(rem(2 * n + j, RING)) * TILE + half * SUB, SUB), SUB)
            here = pl.ds(j * SUB, SUB)
            copies += [
                pltpu.make_async_copy(wg_hbm.at[layer, :, at], WGU.at[slot, :, here], wsem.at[slot, 3 * j]),
                pltpu.make_async_copy(wu_hbm.at[layer, :, at], WGU.at[slot, :, pl.ds(TILE + j * SUB, SUB)], wsem.at[slot, 3 * j + 1]),
                pltpu.make_async_copy(wd_hbm.at[layer, at, :], WD.at[slot, here, :], wsem.at[slot, 3 * j + 2]),
            ]
        return copies

    def start_weights(layer, k):
        for c in weight_copies(layer, k):
            c.start()

    def next_weights(layer, k):
        for c in weight_copies(layer, k):
            c.wait()

        @pl.when(k < RING - 1)
        def _():
            start_weights(layer, k + 1)

    x_copy = pltpu.make_async_copy(x_hbm, H, xsem.at[0])
    dy_copy = pltpu.make_async_copy(dy_hbm, DY, xsem.at[1])
    x_copy.start()
    dy_copy.start()
    start_weights(0, 0)

    barrier = pltpu.get_barrier_semaphore()
    for other in (partner, device(rem(pos + 1, RING), core), device(rem(pos + 7, RING), core)):
        pl.semaphore_signal(barrier, inc=1, device_id=other, device_id_type=MESH)

    def rows(r, n=ROWS):
        return pl.ds(pl.multiple_of(r * n, n), n)

    def normed_into(dst):
        @pl.loop(0, T // FEW)
        def _(r):
            at = rows(r, FEW)
            wide = H[at, :].astype(F32)
            scale = lax.rsqrt(jnp.mean(wide * wide, -1, keepdims=True) + 1e-6)
            dst[at, :] = (wide * scale).astype(BF)

    def transposed_into(dst, src):
        @pl.loop(0, T // FEW)
        def _(r):
            at = rows(r, FEW)
            dst[:, at] = src[at, :].T

    def partner_copy(part, k):
        p = chunk(k)
        return pltpu.make_async_remote_copy(
            src_ref=G.at[part, p, 1 - core], dst_ref=R.at[part, p],
            send_sem=p_s.at[part, k], recv_sem=p_r.at[part, k], device_id=partner, device_id_type=MESH,
        )

    def ring_copy(part, k, m, sign):
        return pltpu.make_async_remote_copy(
            src_ref=R.at[part, chunk(k), m], dst_ref=L.at[part, k, m],
            send_sem=rs_s.at[part, k, m], recv_sem=rs_r.at[part, k, m],
            device_id=device(rem(pos + RING + sign, RING), core), device_id_type=MESH,
        )

    def add_up(part, k, m, came):
        p = chunk(k)

        @pl.loop(0, HALF // 64)
        def _(r):
            at = rows(r, 64)
            total = G[part, p, core, m, at, :].astype(F32) + R[part, p, m, at, :].astype(F32)
            for j in came:
                total += L[part, j, m, at, :].astype(F32)
            R[part, p, m, at, :] = total.astype(BF)

    def reduce_step(part, k):
        partner_copy(part, k).wait()

        @pl.loop(0, 3)
        def _(m):
            @pl.when((k == 0) | ((k == 1) & (core == 1)) | ((k == 2) & (core == 0)))
            def _():
                add_up(part, k, m, ())

            @pl.when((k == 1) & (core == 0) | (k == 2) & (core == 1))
            def _():
                ring_copy(part, 0, m, 1).wait_recv()
                add_up(part, k, m, (0,))

            @pl.when(k >= 3)
            def _():
                ring_copy(part, k - 2, m, 1).wait_recv()
                add_up(part, k, m, (k - 2,))

            @pl.when(k == 0)
            def _():
                ring_copy(part, k, m, 1 - 2 * core).start()

            @pl.when(k > 0)
            def _():
                ring_copy(part, k, m, 2 * rem(k, 2) - 1).start()

    def reduce_last(part):
        partner_copy(part, 7).wait()
        pl.semaphore_signal(free.at[part], inc=1, device_id=partner, device_id_type=MESH)

        @pl.loop(0, 3)
        def _(m):
            ring_copy(part, 5, m, 1).wait_recv()
            ring_copy(part, 6, m, 1).wait_recv()

            @pl.loop(0, HALF // 64)
            def _(r):
                at = rows(r, 64)
                total = G[part, pos, core, m, at, :].astype(F32) + R[part, pos, m, at, :].astype(F32)
                total += L[part, 5, m, at, :].astype(F32)
                total += L[part, 6, m, at, :].astype(F32)
                G[part, pos, core, m, at, :] = total.astype(BF)

            gather_copy(part, 1, m, pos, 1).start()
            gather_copy(part, 2, m, pos, -1).start()

        pl.semaphore_wait(free.at[part], 1)
        share_copy(part, 0, core).start()

    def event_chunk(e):
        return rem(pos + 8 + div(e + 1, 2) * (1 - 2 * rem(e, 2)), RING)

    def gather_copy(part, e, m, p, sign):
        return pltpu.make_async_remote_copy(
            src_ref=G.at[part, p, core, m], dst_ref=G.at[part, p, core, m],
            send_sem=ag_s.at[part, e, m], recv_sem=ag_r.at[part, e, m],
            device_id=device(rem(pos + RING + sign, RING), core), device_id_type=MESH,
        )

    def share_copy(part, e, c):
        p = event_chunk(e)
        return pltpu.make_async_remote_copy(
            src_ref=G.at[part, p, c], dst_ref=G.at[part, p, c],
            send_sem=ap_s.at[part, e], recv_sem=ap_r.at[part, e], device_id=partner, device_id_type=MESH,
        )

    def gather_event(part, e):
        p = event_chunk(e)

        @pl.loop(0, 3)
        def _(m):
            gather_copy(part, e, m, p, 1).wait_recv()

            @pl.when((e <= 4) | ((e == 5) & (core == 0)))
            def _():
                gather_copy(part, e + 2, m, p, 2 * rem(e, 2) - 1).start()

            @pl.when((e == 6) & (core == 1))
            def _():
                gather_copy(part, 7, m, p, -1).start()

        share_copy(part, e, core).start()

    def out_copy(part, e):
        p = event_chunk(e)
        return pltpu.make_async_copy(G.at[part, p], g_out.at[part, p], osem.at[part, e])

    def squares(part, e):
        share_copy(part, e, 1 - core).wait_recv()
        out_copy(part, e).start()
        p = event_chunk(e)
        total = jnp.zeros((8, SUB), F32)
        for c in range(2):

            def add(i, total):
                wide = G[part, p, c, div(i, 5), rows(rem(i, 5), 64), :].astype(F32)
                return total + jnp.sum((wide * wide).reshape(8, 8, SUB), 0)

            total = lax.fori_loop(0, 3 * HALF // 64, add, total)
        PS[part, p] = total

    x_copy.wait()
    normed_into(A)

    @pl.loop(0, RING)
    def _(k):
        next_weights(0, k)
        slot = rem(k, 2)

        @pl.loop(0, T // ROWS)
        def _(r):
            at = rows(r)
            both = dot(A[at, :], WGU[slot], 1, 0)
            gate, up = both[:, :TILE], both[:, TILE:]
            hid = (gate * jax.nn.sigmoid(gate) * up).astype(BF)
            part = dot(hid, WD[slot], 1, 0)

            @pl.when(k == 0)
            def _():
                ACC[at, :] = part

            @pl.when(k > 0)
            def _():
                ACC[at, :] += part

    start_weights(1, 0)

    @pl.loop(0, T // FEW)
    def _(r):
        at = rows(r, FEW)
        H[at, :] = (H[at, :].astype(F32) + ACC[at, :].astype(BF).astype(F32)).astype(BF)

    normed_into(A)
    transposed_into(AT, A)
    dy_copy.wait()
    transposed_into(DYT, DY)

    def tile(layer, n, midway, after):
        part = 2 * (1 - layer) + div(n, 4)
        next_weights(layer, n)
        slot = rem(n, 2)
        if layer == 1:

            @pl.when(n > 1)
            def _():
                keep_copy(n - 2).wait()

        @pl.loop(0, T // ROWS)
        def _(r):
            at = rows(r)
            both = dot(A[at, :], WGU[slot], 1, 0)
            gate, up = both[:, :TILE], both[:, TILE:]
            by_hid = dot(DY[at, :], WD[slot], 1, 1).astype(BF).astype(F32)
            sig = jax.nn.sigmoid(gate)
            silu = gate * sig
            HID[at, :] = (silu * up).astype(BF)
            DGU[slot, at, pl.ds(TILE, TILE)] = (by_hid * silu).astype(BF)
            DGU[slot, at, pl.ds(0, TILE)] = (by_hid * up * (sig + silu * (1.0 - sig))).astype(BF)

        if layer == 1:
            keep_copy(n).start()

        at_turn(n, midway)

        for left, right, ms in ((AT, DGU.at[slot], (0, 1)), (DYT, HID, (2,))):
            g = dot(left[...], right[...], 1, 0).astype(BF)
            for i, m in enumerate(ms):
                for j in range(2):
                    at = slice(i * TILE + j * SUB, i * TILE + (j + 1) * SUB)
                    for half in range(2):
                        G[part, chunk(rem(2 * n + j, RING)), half, m] = g[half * HALF : (half + 1) * HALF, at]

        for j in range(2):
            partner_copy(part, rem(2 * n + j, RING)).start()

        at_turn(n, after)

    def keep_copy(n):
        return pltpu.make_async_copy(DGU.at[rem(n, 2)], kept.at[n], ksem.at[rem(n, 2)])

    def fetch_copy(n):
        return pltpu.make_async_copy(kept.at[n], DGU.at[rem(n, 2)], ksem.at[rem(n, 2)])

    def at_turn(n, then):
        for turn, calls in then.items():

            @pl.when(n == turn)
            def _(calls=calls):
                for call, part, *rest in calls:
                    call(part, *rest)

    def one(call, part, odd):
        return call, part, odd + core

    def other(call, part, odd):
        return call, part, odd + 1 - core

    step_, last, gather = reduce_step, reduce_last, gather_event
    pl.semaphore_wait(barrier, 3)

    @pl.loop(0, RING)
    def _(n):
        tile(
            1, n,
            {
                1: [(step_, 0, 0)],
                3: [other(step_, 0, 1)],
                4: [one(step_, 0, 3)],
                5: [(step_, 1, 0)],
                6: [other(step_, 0, 5)],
                7: [other(step_, 1, 1)],
            },
            {
                2: [one(step_, 0, 1)],
                4: [other(step_, 0, 3)],
                5: [one(step_, 0, 5)],
                6: [one(step_, 1, 1)],
                7: [(last, 0)],
            },
        )

    start_weights(1, 0)
    keep_copy(6).wait()
    fetch_copy(0).start()
    keep_copy(7).wait()

    @pl.loop(0, RING)
    def _(n):
        next_weights(1, n)
        fetch_copy(n).wait()

        @pl.when(n < RING - 1)
        def _():
            fetch_copy(n + 1).start()

        slot = rem(n, 2)

        @pl.loop(0, T // ROWS)
        def _(r):
            at = rows(r)
            term = dot(DGU[slot, at, :], WGU[slot], 1, 1)

            @pl.when(n == 0)
            def _():
                ACC[at, :] = term

            @pl.when(n > 0)
            def _():
                ACC[at, :] += term

        at_turn(n, {
            0: [one(step_, 1, 3)],
            1: [other(step_, 1, 3)],
            2: [one(gather, 0, 1)],
            3: [one(step_, 1, 5), other(gather, 0, 1)],
            4: [other(step_, 1, 5)],
            5: [one(gather, 0, 3)],
            6: [other(gather, 0, 3)],
            7: [(last, 1)],
        })

    start_weights(0, 0)

    @pl.loop(0, T // FEW)
    def _(r):
        at = rows(r, FEW)
        by_a = ACC[at, :].astype(BF).astype(F32)
        wide = H[at, :].astype(F32)
        scale = lax.rsqrt(jnp.mean(wide * wide, -1, keepdims=True) + 1e-6)
        along = jnp.mean(by_a * wide, -1, keepdims=True) * (scale * scale)
        by_h = (scale * (by_a - wide * along)).astype(BF).astype(F32)
        DY[at, :] = (DY[at, :].astype(F32) + by_h).astype(BF)

    again = pltpu.make_async_copy(x_hbm, H, xsem.at[0])
    again.start()
    transposed_into(DYT, DY)
    gather_event(0, 5 + core)
    again.wait()
    normed_into(A)
    transposed_into(AT, A)

    @pl.loop(0, RING)
    def _(n):
        tile(
            0, n,
            {
                0: [other(gather, 0, 5), one(gather, 1, 1)],
                1: [(step_, 2, 0), (gather, 0, 7)],
                2: [other(gather, 1, 3)],
                3: [other(step_, 2, 1), one(gather, 1, 5)],
                4: [one(step_, 2, 3)],
                5: [(step_, 3, 0)],
                6: [other(step_, 2, 5)],
                7: [other(step_, 3, 1)],
            },
            {
                0: [other(gather, 1, 1)],
                1: [one(gather, 1, 3)],
                2: [one(step_, 2, 1)],
                3: [other(gather, 1, 5)],
                4: [other(step_, 2, 3), (gather, 1, 7)],
                5: [one(step_, 2, 5)],
                6: [one(step_, 3, 1)],
                7: [(last, 2), one(step_, 3, 3), other(step_, 3, 3)],
            },
        )

    def all_squares(part, first, end):
        @pl.loop(first, end)
        def _(e):
            squares(part, e)

    def both_ways(call, part, odd):
        call(part, odd + core)
        call(part, odd + 1 - core)

    all_squares(0, 0, 8)
    both_ways(reduce_step, 3, 5)
    both_ways(gather_event, 2, 1)
    all_squares(1, 0, 8)
    reduce_last(3)
    both_ways(gather_event, 2, 3)
    all_squares(2, 0, 3)
    both_ways(gather_event, 3, 1)
    both_ways(gather_event, 2, 5)
    both_ways(gather_event, 3, 3)
    gather_event(2, 7)
    all_squares(2, 3, 7)
    all_squares(3, 0, 3)
    both_ways(gather_event, 3, 5)
    squares(2, 7)
    all_squares(3, 3, 5)
    gather_event(3, 7)
    all_squares(3, 5, 8)

    total = jnp.zeros((8, SUB), F32)
    for part in range(PARTS):
        for p in range(RING):
            total += PS[part, p]
    ss_out[...] = total

    for part in range(PARTS):

        @pl.loop(0, RING)
        def _(k):
            share_copy(part, k, core).wait_send()
            out_copy(part, k).wait()

        @pl.loop(0, RING - 1)
        def _(k):
            for m in range(3):
                ring_copy(part, k, m, 1).wait_send()
                gather_copy(part, k + 1, m, event_chunk(k + 1), 1).wait_send()


def update_kernel(ss, g, *refs):
    ins, outs = refs[:9], refs[9:]
    count = float(3 * LAYERS * D * FF)
    factor = jnp.minimum(1.0, 0.5 * lax.rsqrt(jnp.sum(ss[...]) / count + 1e-30))
    for i in range(3):
        w, m, v = ins[3 * i : 3 * i + 3]
        new_w, new_m, new_v = outs[3 * i : 3 * i + 3]
        grad = jnp.concatenate([g[half, 0, :, i].reshape(D, SUB) for half in range(2)], 1).astype(F32) * factor
        if i == 2:
            grad = grad.T
        mm = 0.9 * m[0] + 0.1 * grad
        vv = 0.95 * v[0] + 0.05 * grad * grad
        wide = w[0].astype(F32)
        new_m[0] = mm
        new_v[0] = vv
        new_w[0] = (wide - 0.02 * (mm * lax.rsqrt(vv + 1e-8) + 0.1 * wide)).astype(BF)


def solution(mesh):
    any_ = pl.BlockSpec(memory_space=pl.ANY)
    chunk_of = (3, HALF, SUB)
    dma = pltpu.SemaphoreType.DMA

    gradients = pl.pallas_call(
        step_kernel,
        name="gradients",
        out_shape=(
            jax.ShapeDtypeStruct((PARTS, RING, 2, *chunk_of), BF),
            jax.ShapeDtypeStruct((8, SUB), F32),
            jax.ShapeDtypeStruct((RING, T, 2 * TILE), BF),
        ),
        in_specs=[any_] * 5,
        out_specs=(any_, pl.BlockSpec(memory_space=pltpu.VMEM), any_),
        scratch_shapes=[
            pltpu.VMEM((T, D), BF), pltpu.VMEM((T, D), BF), pltpu.VMEM((D, T), BF), pltpu.VMEM((T, D), BF), pltpu.VMEM((D, T), BF),
            pltpu.VMEM((T, D), F32),
            pltpu.VMEM((T, TILE), BF), pltpu.VMEM((2, T, 2 * TILE), BF),
            pltpu.VMEM((2, D, 2 * TILE), BF), pltpu.VMEM((2, TILE, D), BF),
            pltpu.VMEM((PARTS, RING, 2, *chunk_of), BF),
            pltpu.VMEM((PARTS, RING, *chunk_of), BF),
            pltpu.VMEM((PARTS, RING - 1, *chunk_of), BF),
            pltpu.VMEM((PARTS, RING, 8, SUB), F32),
            dma((2, 6)), dma((2,)), dma((PARTS, RING)), dma((2,)),
            dma((PARTS, RING)), dma((PARTS, RING)),
            dma((PARTS, RING - 1, 3)), dma((PARTS, RING - 1, 3)),
            dma((PARTS, RING, 3)), dma((PARTS, RING, 3)),
            dma((PARTS, RING)), dma((PARTS, RING)), pltpu.SemaphoreType.REGULAR((PARTS,)),
        ],
        compiler_params=pltpu.CompilerParams(collective_id=0, has_side_effects=True, vmem_limit_bytes=67_043_328),
    )

    wide = pl.BlockSpec((1, D, TILE), lambda l, p: (l, 0, p))
    tall = pl.BlockSpec((1, TILE, D), lambda l, p: (l, p, 0))
    specs = [wide] * 6 + [tall] * 3
    up_shape, down_shape = (LAYERS, D, FF), (LAYERS, FF, D)
    shapes = [jax.ShapeDtypeStruct(s, t) for s in (up_shape, up_shape, down_shape) for t in (BF, F32, F32)]
    update = pl.pallas_call(
        update_kernel,
        name="update",
        grid=(LAYERS, RING),
        out_shape=shapes,
        in_specs=[pl.BlockSpec((8, SUB), lambda l, p: (0, 0)), pl.BlockSpec((2, 1, 2, *chunk_of), lambda l, p: (1 - l, p, 0, 0, 0, 0))] + specs,
        out_specs=specs,
        compiler_params=pltpu.CompilerParams(vmem_limit_bytes=60_000_000),
    )

    def step(x, dy, wg, wu, wd, mg, mu, md, vg, vu, vd):
        g, ss, _ = gradients(x[0], dy[0], wg, wu, wd)
        new = update(ss, g, wg, mg, vg, wu, mu, vu, wd, md, vd)
        return tuple(new[3 * i + which] for which in range(3) for i in range(3))

    return jax.shard_map(
        step,
        mesh=mesh,
        in_specs=(P(("rep", "dp"), None, None),) * 2 + (P(None, None, None),) * 9,
        out_specs=(P("rep", None, None),) * 9,
        check_vma=False,
    )
```

```python
import jax
import jax.numpy as jnp
from jax import lax
from jax.experimental import pallas as pl
from jax.experimental.pallas import tpu as pltpu
from jax.sharding import PartitionSpec as P

T, D, FF, LAYERS = 2048, 640, 2048, 2
RING = 8
TILE = FF // RING
HALF = D // 2
SUB = TILE // 2
PARTS = 2 * LAYERS
ROWS, FEW = 1024, 512
BF, F32 = jnp.bfloat16, jnp.float32
MESH = pl.DeviceIdType.MESH


def rem(a, b):
    return a % b if isinstance(a, int) else lax.rem(a, jnp.int32(b))


def div(a, b):
    return a // b if isinstance(a, int) else lax.div(a, jnp.int32(b))


def dot(a, b, ca, cb):
    return lax.dot_general(a, b, (((ca,), (cb,)), ((), ())), preferred_element_type=F32)


def step_kernel(
    x_hbm, dy_hbm, wg_hbm, wu_hbm, wd_hbm, g_out, ss_out, kept,
    H, A, AT, DY, DYT, ACC, HID, DGU, WGU, WD, G, R, L, PS,
    wsem, xsem, osem, ksem, p_s, p_r, rs_s, rs_r, ag_s, ag_r, ap_s, ap_r, free,
):
    me = lax.axis_index("dp")
    core = rem(me, 2)
    y, z = div(me, 8), rem(div(me, 2), 4)
    pos = z + y * (7 - 2 * z)

    def device(position, c):
        yy = div(position, 4)
        zz = position - yy * (2 * position - 7)
        return {"dp": yy * 8 + zz * 2 + c}

    partner = device(pos, 1 - core)

    def chunk(k):
        return rem(pos + 8 + (4 - div(k + 1, 2)) * (2 * rem(k, 2) - 1), RING)

    def weight_copies(layer, n):
        slot, half = rem(n, 2), div(n, 4)
        copies = []
        for j in range(2):
            at = pl.ds(pl.multiple_of(chunk(rem(2 * n + j, RING)) * TILE + half * SUB, SUB), SUB)
            here = pl.ds(j * SUB, SUB)
            copies += [
                pltpu.make_async_copy(wg_hbm.at[layer, :, at], WGU.at[slot, :, here], wsem.at[slot, 3 * j]),
                pltpu.make_async_copy(wu_hbm.at[layer, :, at], WGU.at[slot, :, pl.ds(TILE + j * SUB, SUB)], wsem.at[slot, 3 * j + 1]),
                pltpu.make_async_copy(wd_hbm.at[layer, at, :], WD.at[slot, here, :], wsem.at[slot, 3 * j + 2]),
            ]
        return copies

    def start_weights(layer, k):
        for c in weight_copies(layer, k):
            c.start()

    def next_weights(layer, k):
        for c in weight_copies(layer, k):
            c.wait()

        @pl.when(k < RING - 1)
        def _():
            start_weights(layer, k + 1)

    x_copy = pltpu.make_async_copy(x_hbm, H, xsem.at[0])
    dy_copy = pltpu.make_async_copy(dy_hbm, DY, xsem.at[1])
    x_copy.start()
    dy_copy.start()
    start_weights(0, 0)

    barrier = pltpu.get_barrier_semaphore()
    for other in (partner, device(rem(pos + 1, RING), core), device(rem(pos + 7, RING), core)):
        pl.semaphore_signal(barrier, inc=1, device_id=other, device_id_type=MESH)

    def rows(r, n=ROWS):
        return pl.ds(pl.multiple_of(r * n, n), n)

    def normed_into(dst):
        @pl.loop(0, T // FEW)
        def _(r):
            at = rows(r, FEW)
            wide = H[at, :].astype(F32)
            scale = lax.rsqrt(jnp.mean(wide * wide, -1, keepdims=True) + 1e-6)
            dst[at, :] = (wide * scale).astype(BF)

    def transposed_into(dst, src):
        @pl.loop(0, T // FEW)
        def _(r):
            at = rows(r, FEW)
            dst[:, at] = src[at, :].T

    def partner_copy(part, k):
        p = chunk(k)
        return pltpu.make_async_remote_copy(
            src_ref=G.at[part, p, 1 - core], dst_ref=R.at[part, p],
            send_sem=p_s.at[part, k], recv_sem=p_r.at[part, k], device_id=partner, device_id_type=MESH,
        )

    def ring_copy(part, k, m, sign):
        return pltpu.make_async_remote_copy(
            src_ref=R.at[part, chunk(k), m], dst_ref=L.at[part, k, m],
            send_sem=rs_s.at[part, k, m], recv_sem=rs_r.at[part, k, m],
            device_id=device(rem(pos + RING + sign, RING), core), device_id_type=MESH,
        )

    def add_up(part, k, m, came):
        p = chunk(k)

        @pl.loop(0, HALF // 64)
        def _(r):
            at = rows(r, 64)
            total = G[part, p, core, m, at, :].astype(F32) + R[part, p, m, at, :].astype(F32)
            for j in came:
                total += L[part, j, m, at, :].astype(F32)
            R[part, p, m, at, :] = total.astype(BF)

    def reduce_step(part, k):
        partner_copy(part, k).wait()

        @pl.loop(0, 3)
        def _(m):
            @pl.when((k == 0) | ((k == 1) & (core == 1)) | ((k == 2) & (core == 0)))
            def _():
                add_up(part, k, m, ())

            @pl.when((k == 1) & (core == 0) | (k == 2) & (core == 1))
            def _():
                ring_copy(part, 0, m, 1).wait_recv()
                add_up(part, k, m, (0,))

            @pl.when(k >= 3)
            def _():
                ring_copy(part, k - 2, m, 1).wait_recv()
                add_up(part, k, m, (k - 2,))

            @pl.when(k == 0)
            def _():
                ring_copy(part, k, m, 1 - 2 * core).start()

            @pl.when(k > 0)
            def _():
                ring_copy(part, k, m, 2 * rem(k, 2) - 1).start()

    def reduce_last(part):
        partner_copy(part, 7).wait()
        pl.semaphore_signal(free.at[part], inc=1, device_id=partner, device_id_type=MESH)

        @pl.loop(0, 3)
        def _(m):
            ring_copy(part, 5, m, 1).wait_recv()
            ring_copy(part, 6, m, 1).wait_recv()

            @pl.loop(0, HALF // 64)
            def _(r):
                at = rows(r, 64)
                total = G[part, pos, core, m, at, :].astype(F32) + R[part, pos, m, at, :].astype(F32)
                total += L[part, 5, m, at, :].astype(F32)
                total += L[part, 6, m, at, :].astype(F32)
                G[part, pos, core, m, at, :] = total.astype(BF)

            gather_copy(part, 1, m, pos, 1).start()
            gather_copy(part, 2, m, pos, -1).start()

        pl.semaphore_wait(free.at[part], 1)
        share_copy(part, 0, core).start()

    def event_chunk(e):
        return rem(pos + 8 + div(e + 1, 2) * (1 - 2 * rem(e, 2)), RING)

    def gather_copy(part, e, m, p, sign):
        return pltpu.make_async_remote_copy(
            src_ref=G.at[part, p, core, m], dst_ref=G.at[part, p, core, m],
            send_sem=ag_s.at[part, e, m], recv_sem=ag_r.at[part, e, m],
            device_id=device(rem(pos + RING + sign, RING), core), device_id_type=MESH,
        )

    def share_copy(part, e, c):
        p = event_chunk(e)
        return pltpu.make_async_remote_copy(
            src_ref=G.at[part, p, c], dst_ref=G.at[part, p, c],
            send_sem=ap_s.at[part, e], recv_sem=ap_r.at[part, e], device_id=partner, device_id_type=MESH,
        )

    def gather_event(part, e):
        p = event_chunk(e)

        @pl.loop(0, 3)
        def _(m):
            gather_copy(part, e, m, p, 1).wait_recv()

            @pl.when((e <= 4) | ((e == 5) & (core == 0)))
            def _():
                gather_copy(part, e + 2, m, p, 2 * rem(e, 2) - 1).start()

            @pl.when((e == 6) & (core == 1))
            def _():
                gather_copy(part, 7, m, p, -1).start()

        share_copy(part, e, core).start()

    def out_copy(part, e):
        p = event_chunk(e)
        return pltpu.make_async_copy(G.at[part, p], g_out.at[part, p], osem.at[part, e])

    def squares(part, e):
        share_copy(part, e, 1 - core).wait_recv()
        out_copy(part, e).start()
        p = event_chunk(e)
        total = jnp.zeros((8, SUB), F32)
        for c in range(2):

            def add(m, total):
                wide = G[part, p, c, m].astype(F32)
                return total + jnp.sum((wide * wide).reshape(HALF // 8, 8, SUB), 0)

            total = lax.fori_loop(0, 3, add, total)
        PS[part, p] = total

    x_copy.wait()
    normed_into(A)

    @pl.loop(0, RING)
    def _(k):
        next_weights(0, k)
        slot = rem(k, 2)

        @pl.loop(0, T // 2048)
        def _(r):
            at = rows(r, 2048)
            both = dot(A[at, :], WGU[slot], 1, 0)
            gate, up = both[:, :TILE], both[:, TILE:]
            hid = (gate * jax.nn.sigmoid(gate) * up).astype(BF)
            part = dot(hid, WD[slot], 1, 0)

            @pl.when(k == 0)
            def _():
                ACC[at, :] = part

            @pl.when(k > 0)
            def _():
                ACC[at, :] += part

    start_weights(1, 0)

    @pl.loop(0, T // FEW)
    def _(r):
        at = rows(r, FEW)
        H[at, :] = (H[at, :].astype(F32) + ACC[at, :].astype(BF).astype(F32)).astype(BF)

    normed_into(A)
    transposed_into(AT, A)
    dy_copy.wait()
    transposed_into(DYT, DY)

    def tile(layer, n, midway, after):
        part = 2 * (1 - layer) + div(n, 4)
        next_weights(layer, n)
        slot = rem(n, 2)
        if layer == 1:

            @pl.when(n > 1)
            def _():
                keep_copy(n - 2).wait()

        @pl.loop(0, T // ROWS)
        def _(r):
            at = rows(r)
            both = dot(A[at, :], WGU[slot], 1, 0)
            gate, up = both[:, :TILE], both[:, TILE:]
            by_hid = dot(DY[at, :], WD[slot], 1, 1).astype(BF).astype(F32)
            sig = jax.nn.sigmoid(gate)
            silu = gate * sig
            HID[at, :] = (silu * up).astype(BF)
            DGU[slot, at, pl.ds(TILE, TILE)] = (by_hid * silu).astype(BF)
            DGU[slot, at, pl.ds(0, TILE)] = (by_hid * up * (sig + silu * (1.0 - sig))).astype(BF)

        if layer == 1:
            keep_copy(n).start()

        at_turn(n, midway)

        for left, right, ms in ((AT, DGU.at[slot], (0, 1)), (DYT, HID, (2,))):
            g = dot(left[...], right[...], 1, 0).astype(BF)
            for i, m in enumerate(ms):
                for j in range(2):
                    at = slice(i * TILE + j * SUB, i * TILE + (j + 1) * SUB)
                    for half in range(2):
                        G[part, chunk(rem(2 * n + j, RING)), half, m] = g[half * HALF : (half + 1) * HALF, at]

        for j in range(2):
            partner_copy(part, rem(2 * n + j, RING)).start()

        at_turn(n, after)

    def keep_copy(n):
        return pltpu.make_async_copy(DGU.at[rem(n, 2)], kept.at[n], ksem.at[rem(n, 2)])

    def fetch_copy(n):
        return pltpu.make_async_copy(kept.at[n], DGU.at[rem(n, 2)], ksem.at[rem(n, 2)])

    def at_turn(n, then):
        for turn, calls in then.items():

            @pl.when(n == turn)
            def _(calls=calls):
                for call, part, *rest in calls:
                    call(part, *rest)

    def one(call, part, odd):
        return call, part, odd + core

    def other(call, part, odd):
        return call, part, odd + 1 - core

    step_, last, gather = reduce_step, reduce_last, gather_event
    pl.semaphore_wait(barrier, 3)

    @pl.loop(0, RING)
    def _(n):
        tile(
            1, n,
            {
                1: [(step_, 0, 0)],
                3: [other(step_, 0, 1)],
                4: [one(step_, 0, 3)],
                5: [(step_, 1, 0)],
                6: [other(step_, 0, 5)],
                7: [other(step_, 1, 1)],
            },
            {
                2: [one(step_, 0, 1)],
                4: [other(step_, 0, 3)],
                5: [one(step_, 0, 5)],
                6: [one(step_, 1, 1)],
                7: [(last, 0)],
            },
        )

    start_weights(1, 0)
    keep_copy(6).wait()
    fetch_copy(0).start()
    keep_copy(7).wait()

    @pl.loop(0, RING)
    def _(n):
        next_weights(1, n)
        fetch_copy(n).wait()

        @pl.when(n < RING - 1)
        def _():
            fetch_copy(n + 1).start()

        slot = rem(n, 2)

        @pl.loop(0, T // ROWS)
        def _(r):
            at = rows(r)
            term = dot(DGU[slot, at, :], WGU[slot], 1, 1)

            @pl.when(n == 0)
            def _():
                ACC[at, :] = term

            @pl.when(n > 0)
            def _():
                ACC[at, :] += term

        at_turn(n, {
            0: [one(step_, 1, 3)],
            1: [other(step_, 1, 3)],
            2: [one(gather, 0, 1)],
            3: [one(step_, 1, 5), other(gather, 0, 1)],
            4: [other(step_, 1, 5)],
            5: [one(gather, 0, 3)],
            6: [other(gather, 0, 3)],
            7: [(last, 1)],
        })

    start_weights(0, 0)

    @pl.loop(0, T // FEW)
    def _(r):
        at = rows(r, FEW)
        by_a = ACC[at, :].astype(BF).astype(F32)
        wide = H[at, :].astype(F32)
        scale = lax.rsqrt(jnp.mean(wide * wide, -1, keepdims=True) + 1e-6)
        along = jnp.mean(by_a * wide, -1, keepdims=True) * (scale * scale)
        by_h = (scale * (by_a - wide * along)).astype(BF).astype(F32)
        DY[at, :] = (DY[at, :].astype(F32) + by_h).astype(BF)

    again = pltpu.make_async_copy(x_hbm, H, xsem.at[0])
    again.start()
    transposed_into(DYT, DY)
    gather_event(0, 5 + core)
    again.wait()
    normed_into(A)
    transposed_into(AT, A)

    @pl.loop(0, RING)
    def _(n):
        tile(
            0, n,
            {
                0: [other(gather, 0, 5), one(gather, 1, 1)],
                1: [(step_, 2, 0), (gather, 0, 7)],
                2: [one(step_, 2, 1), other(gather, 1, 3)],
                3: [one(step_, 2, 3), one(gather, 1, 5)],
                4: [one(step_, 2, 5)],
                5: [(step_, 3, 0), (gather, 1, 7)],
                6: [one(step_, 3, 1)],
                7: [one(step_, 3, 3), one(gather, 2, 1)],
            },
            {
                0: [other(gather, 1, 1)],
                1: [one(gather, 1, 3)],
                2: [other(step_, 2, 1)],
                3: [other(step_, 2, 3), other(gather, 1, 5)],
                4: [other(step_, 2, 5)],
                5: [(last, 2)],
                6: [other(step_, 3, 1)],
                7: [other(step_, 3, 3), other(gather, 2, 1)],
            },
        )

    def all_squares(part, first, end):
        @pl.loop(first, end)
        def _(e):
            squares(part, e)

    def both_ways(call, part, odd):
        call(part, odd + core)
        call(part, odd + 1 - core)

    all_squares(0, 0, 8)
    both_ways(reduce_step, 3, 5)
    all_squares(1, 0, 6)
    both_ways(gather_event, 2, 3)
    reduce_last(3)
    all_squares(1, 6, 8)
    both_ways(gather_event, 2, 5)
    all_squares(2, 0, 3)
    both_ways(gather_event, 3, 1)
    gather_event(2, 7)
    all_squares(2, 3, 5)
    both_ways(gather_event, 3, 3)
    all_squares(2, 5, 7)
    all_squares(3, 0, 3)
    both_ways(gather_event, 3, 5)
    squares(2, 7)
    all_squares(3, 3, 5)
    gather_event(3, 7)
    all_squares(3, 5, 8)

    total = jnp.zeros((8, SUB), F32)
    for part in range(PARTS):
        for p in range(RING):
            total += PS[part, p]
    ss_out[...] = total

    for part in range(PARTS):

        @pl.loop(0, RING)
        def _(k):
            share_copy(part, k, core).wait_send()
            out_copy(part, k).wait()

        @pl.loop(0, RING - 1)
        def _(k):
            for m in range(3):
                ring_copy(part, k, m, 1).wait_send()
                gather_copy(part, k + 1, m, event_chunk(k + 1), 1).wait_send()


def update_kernel(ss, g, *refs):
    ins, outs = refs[:9], refs[9:]
    count = float(3 * LAYERS * D * FF)
    factor = jnp.minimum(1.0, 0.5 * lax.rsqrt(jnp.sum(ss[...]) / count + 1e-30))
    for i in range(3):
        w, m, v = ins[3 * i : 3 * i + 3]
        new_w, new_m, new_v = outs[3 * i : 3 * i + 3]
        grad = jnp.concatenate([g[half, 0, :, i].reshape(D, SUB) for half in range(2)], 1).astype(F32) * factor
        if i == 2:
            grad = grad.T
        mm = 0.9 * m[0] + 0.1 * grad
        vv = 0.95 * v[0] + 0.05 * grad * grad
        wide = w[0].astype(F32)
        new_m[0] = mm
        new_v[0] = vv
        new_w[0] = (wide - 0.02 * (mm * lax.rsqrt(vv + 1e-8) + 0.1 * wide)).astype(BF)


def solution(mesh):
    any_ = pl.BlockSpec(memory_space=pl.ANY)
    chunk_of = (3, HALF, SUB)
    dma = pltpu.SemaphoreType.DMA

    gradients = pl.pallas_call(
        step_kernel,
        name="gradients",
        out_shape=(
            jax.ShapeDtypeStruct((PARTS, RING, 2, *chunk_of), BF),
            jax.ShapeDtypeStruct((8, SUB), F32),
            jax.ShapeDtypeStruct((RING, T, 2 * TILE), BF),
        ),
        in_specs=[any_] * 5,
        out_specs=(any_, pl.BlockSpec(memory_space=pltpu.VMEM), any_),
        scratch_shapes=[
            pltpu.VMEM((T, D), BF), pltpu.VMEM((T, D), BF), pltpu.VMEM((D, T), BF), pltpu.VMEM((T, D), BF), pltpu.VMEM((D, T), BF),
            pltpu.VMEM((T, D), F32),
            pltpu.VMEM((T, TILE), BF), pltpu.VMEM((2, T, 2 * TILE), BF),
            pltpu.VMEM((2, D, 2 * TILE), BF), pltpu.VMEM((2, TILE, D), BF),
            pltpu.VMEM((PARTS, RING, 2, *chunk_of), BF),
            pltpu.VMEM((PARTS, RING, *chunk_of), BF),
            pltpu.VMEM((PARTS, RING - 1, *chunk_of), BF),
            pltpu.VMEM((PARTS, RING, 8, SUB), F32),
            dma((2, 6)), dma((2,)), dma((PARTS, RING)), dma((2,)),
            dma((PARTS, RING)), dma((PARTS, RING)),
            dma((PARTS, RING - 1, 3)), dma((PARTS, RING - 1, 3)),
            dma((PARTS, RING, 3)), dma((PARTS, RING, 3)),
            dma((PARTS, RING)), dma((PARTS, RING)), pltpu.SemaphoreType.REGULAR((PARTS,)),
        ],
        compiler_params=pltpu.CompilerParams(collective_id=0, has_side_effects=True, vmem_limit_bytes=67_043_328),
    )

    wide = pl.BlockSpec((1, D, TILE), lambda l, p: (l, 0, p))
    tall = pl.BlockSpec((1, TILE, D), lambda l, p: (l, p, 0))
    specs = [wide] * 6 + [tall] * 3
    up_shape, down_shape = (LAYERS, D, FF), (LAYERS, FF, D)
    shapes = [jax.ShapeDtypeStruct(s, t) for s in (up_shape, up_shape, down_shape) for t in (BF, F32, F32)]
    update = pl.pallas_call(
        update_kernel,
        name="update",
        grid=(LAYERS, RING),
        out_shape=shapes,
        in_specs=[pl.BlockSpec((8, SUB), lambda l, p: (0, 0)), pl.BlockSpec((2, 1, 2, *chunk_of), lambda l, p: (1 - l, p, 0, 0, 0, 0))] + specs,
        out_specs=specs,
        compiler_params=pltpu.CompilerParams(vmem_limit_bytes=60_000_000),
    )

    def step(x, dy, wg, wu, wd, mg, mu, md, vg, vu, vd):
        g, ss, _ = gradients(x[0], dy[0], wg, wu, wd)
        new = update(ss, g, wg, mg, vg, wu, mu, vu, wd, md, vd)
        return tuple(new[3 * i + which] for which in range(3) for i in range(3))

    return jax.shard_map(
        step,
        mesh=mesh,
        in_specs=(P(("rep", "dp"), None, None),) * 2 + (P(None, None, None),) * 9,
        out_specs=(P("rep", None, None),) * 9,
        check_vma=False,
    )
```
